256 devices in a mesh: cp: 64 (over z_hi, y, x, core), tp: 4 (over z_lo).
Axes of the slice: x: 4, y: 4, z: 8 (z_hi: 2, z_lo: 4; z = z_hi * 4 + z_lo), core: 2. Of those that a mesh axis runs over, the one named last changes fastest.
Arguments:
- queries: bfloat16 [49152, 5120], P('cp', 'tp'), may hold values from -36 to 36
- keys: bfloat16 [49152, 1024], P('cp', 'tp'), may hold values from -5 to 5
- values: bfloat16 [49152, 1024], P('cp', 'tp'), may hold values from -6 to 6
- doc_lengths: int32 [64], replicated, may hold values from 1 to 1536, 49152 in all
Outputs:
- attended: bfloat16 [49152, 5120], P(('cp', 'tp'))
The draws below stay inside these ranges and needn't reach their ends.
Inputs may be any that keep to these rules, and one draw needn't show every extreme that they name: `doc_lengths`: they sum to 49152, and one of them is exactly 1536.
All inputs are finite; a program needn't handle non-finite values.
Results may differ from the reference program's by a relative error of at most 0.0038.
Values may be sent and summed in bfloat16 or wider, within the bound.
No kernel may reach another device: no remote copies, remote signals or barrier semaphores. Data moves between devices by JAX's collectives and lax.ppermute only.
A program may use at most 256 MiB of HBM per device.

```python
import math
import jax
import jax.numpy as jnp
import numpy as np
from jax import lax

Q_HEADS = 40
KV_HEADS = 8
HEAD = 128
TOK_DEV = 768
TOKENS = 49152
MAXDOC = 1536
NDOCS = 64
N_CP = 64


def draw_keys(key, part):
    drawn_draw = jnp.clip(jax.random.normal(jax.random.fold_in(key, 11), (TOKENS, KV_HEADS, HEAD), jnp.float32), -5.0, 5.0)
    result = drawn_draw
    return result.reshape(TOKENS, KV_HEADS * HEAD).astype(jnp.bfloat16)


def draw_queries(key, part):
    group_size = Q_HEADS // KV_HEADS
    drawn_draw = jnp.clip(jax.random.normal(jax.random.fold_in(key, 12), (TOKENS, KV_HEADS, group_size, HEAD), jnp.float32), -5.0, 5.0)
    result = drawn_draw
    return result.reshape(TOKENS, Q_HEADS * HEAD).astype(jnp.bfloat16)


def shard_levels(key, dims, split, low, largest):
    loudness, own = 1.0, jax.random.fold_in(key, 6)
    for dim, blocks in split:
        steps = jnp.exp(jax.random.uniform(jax.random.fold_in(own, dim), (blocks,), jnp.float32, low / len(split), largest / len(split)))
        loudness = loudness * jnp.repeat(steps, dims[dim] // blocks).reshape([-1 if axis == dim else 1 for axis in range(len(dims))])
    return loudness


def length_profile(number_of, total, most, slope):
    loads = [(1 << 20) // math.isqrt(standing ** slope) + 1 for standing in range(2, number_of + 1)]
    spare, counts = total - most - (number_of - 1), [1] * (number_of - 1)
    while spare > 0:
        candidates = [i for i in range(number_of - 1) if counts[i] < most]
        mass, left = sum([loads[i] for i in candidates]), spare
        for i in candidates:
            extra = min(most - counts[i], max(1, left * loads[i] // mass), spare)
            counts[i] = counts[i] + extra
            spare = spare - extra
    return np.array([most] + counts)


def ragged_sizes(own_key, amount, total, reach, skew):
    if amount == 2:
        one = jax.random.randint(own_key, (), max(1, total - reach), min(reach, total - 1) + 1)
        return jnp.stack([one, total - one])
    tallies = jnp.asarray(length_profile(amount, total, reach, skew), jnp.int32)
    twos = (amount - 1) // 2
    donor, receiver = tallies[1:1 + 2 * twos:2], tallies[2:2 + 2 * twos:2]
    margin = jnp.minimum(donor - 1, reach - receiver)
    passed = jax.random.randint(jax.random.fold_in(own_key, 1), (twos,), 0, 1 << 20) % (margin + 1)
    tallies = tallies.at[1:1 + 2 * twos:2].set(donor - passed).at[2:2 + 2 * twos:2].set(receiver + passed)
    return tallies[jax.random.permutation(jax.random.fold_in(own_key, 2), amount)]


def bell_draw(own_key, extent, width, most, split=(), held_as=jnp.bfloat16):
    values = jax.random.normal(own_key, extent, jnp.float32) * width
    if len(split) > 0:
        values = shard_levels(own_key, extent, split, -0.22, 0.18) * values
    return jnp.clip(values, min=-most, max=most).astype(held_as)


def setup_inputs(seed: int = 0) -> dict:
    splits = jax.random.split(jax.random.key(seed), 5)
    return {
        "queries": draw_queries(jax.random.fold_in(splits[4], 71), 0),
        "keys": draw_keys(jax.random.fold_in(splits[4], 71), 0),
        "values": bell_draw(splits[2], (TOKENS, KV_HEADS * HEAD), 1.0, 6.0, ((0, 64), (1, 4))),
        "doc_lengths": ragged_sizes(splits[3], NDOCS, TOKENS, MAXDOC, 2).astype(jnp.int32),
    }


negative = -1.0e30


def to_sequence(blocked):
    key_width = blocked.shape[1]
    parts = blocked.reshape(N_CP, 2, TOK_DEV // 2, key_width)
    return jnp.concatenate([parts[:, 0], parts[::-1, 1]], axis=0).reshape(TOKENS, key_width)


def reference(queries, keys, values, doc_lengths):
    half_rows = TOK_DEV // 2
    group_size = Q_HEADS // KV_HEADS
    seq_queries = to_sequence(queries).reshape(TOKENS, KV_HEADS, group_size, HEAD)
    seq_keys = to_sequence(keys).reshape(TOKENS, KV_HEADS, HEAD)
    seq_values = to_sequence(values).reshape(TOKENS, KV_HEADS, HEAD)
    doc_ends = jnp.cumsum(doc_lengths).astype(jnp.int32)
    positions = jnp.arange(TOKENS, dtype=jnp.int32)
    doc_ids = jnp.sum((positions[:, None] >= doc_ends[None, :]).astype(jnp.int32), axis=1).astype(jnp.int32)
    padded_keys = jnp.concatenate([jnp.zeros((MAXDOC, KV_HEADS, HEAD), seq_keys.dtype), seq_keys], axis=0)
    padded_values = jnp.concatenate([jnp.zeros((MAXDOC, KV_HEADS, HEAD), seq_values.dtype), seq_values], axis=0)
    padded_docs = jnp.concatenate([jnp.full((MAXDOC,), -1, jnp.int32), doc_ids], axis=0)
    key_width = MAXDOC + half_rows
    scale = float(HEAD) ** -0.5

    def one_block(block_index):
        row_start = (block_index * half_rows).astype(jnp.int32)
        query_block = lax.dynamic_slice_in_dim(seq_queries, row_start, half_rows, 0)
        key_block = lax.dynamic_slice_in_dim(padded_keys, row_start, key_width, 0)
        value_block = lax.dynamic_slice_in_dim(padded_values, row_start, key_width, 0)
        q_doc = lax.dynamic_slice_in_dim(doc_ids, row_start, half_rows, 0)
        k_doc = lax.dynamic_slice_in_dim(padded_docs, row_start, key_width, 0)
        q_pos = row_start + jnp.arange(half_rows, dtype=jnp.int32)
        k_pos = row_start - MAXDOC + jnp.arange(key_width, dtype=jnp.int32)
        allowed = (k_doc[None, :] == q_doc[:, None]) & (k_pos[None, :] <= q_pos[:, None])
        scores = jnp.einsum("qhjd,khd->qhjk", query_block.astype(jnp.float32), key_block.astype(jnp.float32)) * scale
        allowed_wide = allowed[:, None, None, :]
        masked = jnp.where(allowed_wide, scores, negative)
        row_max = jnp.max(masked, axis=-1, keepdims=True)
        weights = jnp.where(allowed_wide, jnp.exp(masked - row_max), 0.0)
        weight_sum = jnp.sum(weights, axis=-1)
        rounded = lax.optimization_barrier(weights.astype(jnp.bfloat16)).astype(jnp.float32)
        output = jnp.einsum("qhjk,khd->qhjd", rounded, value_block.astype(jnp.float32)) / weight_sum[..., None]
        return output.astype(jnp.bfloat16)

    blocks = lax.map(one_block, jnp.arange(2 * N_CP, dtype=jnp.int32))
    flattened = blocks.reshape(2 * N_CP, half_rows, Q_HEADS * HEAD)
    first_half = flattened[:N_CP]
    second_half = flattened[N_CP:][::-1]
    return jnp.stack([first_half, second_half], axis=1).reshape(TOKENS, Q_HEADS * HEAD)
```

```python
import functools

import jax
import jax.numpy as jnp
from jax import lax
from jax.experimental import pallas as pl
from jax.experimental.pallas import tpu as pltpu
from jax.sharding import PartitionSpec as P

HEAD = 128
TK = 256
PAD = 128
negative = -1e30


def device_of(stretch, cp_size):
    if stretch < cp_size // 2:
        return 2 * stretch
    return 2 * (cp_size - 1 - stretch) + 1


def attend_kernel(group, tile_rows, tiles, bounds, starts, q_ref, k0, k1, k2, v0, v1, v2, o_ref, kbuf, vbuf, m_ref, l_ref, acc_ref):
    index = pl.program_id(0)
    rows = k0.shape[0]
    base = PAD + 2 * rows

    @pl.when(index == 0)
    def fill():
        for buf, parts in ((kbuf, (k2, k1, k0)), (vbuf, (v2, v1, v0))):
            buf[pl.ds(0, PAD), :] = jnp.zeros((PAD, HEAD), buf.dtype)
            for n, part in enumerate(parts):
                buf[pl.ds(PAD + n * rows, rows), :] = part[...]

    first_start = bounds[2 * index]
    last_start = bounds[2 * index + 1]
    tile_first = base + index * tile_rows
    tile_end = tile_first + tile_rows
    steps = (tile_end - first_start + TK - 1) // TK
    factor = float(HEAD) ** (-0.5) * 1.4426950408889634

    def tile(step, masked, opening):
        k_first = pl.multiple_of(tile_end - TK * (step + 1), 64)
        keys = kbuf[pl.ds(k_first, TK), :]
        values = vbuf[pl.ds(k_first, TK), :]
        if masked:
            lanes = k_first + lax.broadcasted_iota(jnp.int32, (tile_rows, TK), 1)
            begin = starts[...]
            begin = jnp.concatenate([begin] * (TK // 128), axis=1)
            allowed = lanes >= begin
            if opening:
                own = tile_first + lax.broadcasted_iota(jnp.int32, (tile_rows, TK), 0)
                allowed = allowed & (lanes <= own)
            bias = jnp.where(allowed, 0.0, negative)
        for j in range(group):
            part = pl.ds(j * tile_rows, tile_rows)
            scores = lax.dot_general(
                q_ref[:, j * HEAD : (j + 1) * HEAD], keys, (((1,), (1,)), ((), ())),
                preferred_element_type=jnp.float32,
            )
            if masked:
                scores = scores + bias
            top = jnp.max(scores, axis=1, keepdims=True)
            if opening:
                new_max = jnp.broadcast_to(top, (tile_rows, HEAD))
            else:
                old_max = m_ref[part, :]
                new_max = jnp.maximum(old_max, top)
                keep = jnp.exp2((old_max - new_max) * factor)
            pieces = [
                jnp.exp2((scores[:, n * 128 : (n + 1) * 128] - new_max) * factor)
                for n in range(TK // 128)
            ]
            total = functools.reduce(jnp.add, pieces)
            weights = jnp.concatenate(pieces, axis=1).astype(jnp.bfloat16)
            product = jnp.dot(weights, values, preferred_element_type=jnp.float32)
            m_ref[part, :] = new_max
            if opening:
                l_ref[part, :] = total
                acc_ref[part, :] = product
            else:
                l_ref[part, :] = keep * l_ref[part, :] + total
                acc_ref[part, :] = keep * acc_ref[part, :] + product

    tile(0, True, True)

    def later(step, carry):
        cut = tile_end - TK * (step + 1) < last_start

        @pl.when(cut)
        def with_mask():
            tile(step, True, False)

        @pl.when(jnp.logical_not(cut))
        def without_mask():
            tile(step, False, False)

        return carry

    lax.fori_loop(1, steps, later, 0)
    for j in range(group):
        part = pl.ds(j * tile_rows, tile_rows)
        total = jnp.sum(l_ref[part, :], axis=1, keepdims=True)
        o_ref[0, :, j * HEAD : (j + 1) * HEAD] = (acc_ref[part, :] / total).astype(o_ref.dtype)


def attend(queries, keys, values, bounds, starts, tiles):
    rows, cols = queries.shape
    tile_rows = rows // tiles
    group = cols // HEAD
    whole = pl.BlockSpec((rows, HEAD), lambda i, b: (0, 0))
    span = PAD + 3 * rows
    return pl.pallas_call(
        functools.partial(attend_kernel, group, tile_rows, tiles),
        grid_spec=pltpu.PrefetchScalarGridSpec(
            num_scalar_prefetch=1,
            grid=(tiles,),
            in_specs=[
                pl.BlockSpec((tile_rows, 128), lambda i, b: (i, 0)),
                pl.BlockSpec((tile_rows, cols), lambda i, b: (i, 0)),
            ]
            + [whole] * 6,
            out_specs=pl.BlockSpec((1, tile_rows, cols), lambda i, b: (i, 0, 0)),
            scratch_shapes=[
                pltpu.VMEM((span, HEAD), jnp.bfloat16),
                pltpu.VMEM((span, HEAD), jnp.bfloat16),
                pltpu.VMEM((group * tile_rows, HEAD), jnp.float32),
                pltpu.VMEM((group * tile_rows, HEAD), jnp.float32),
                pltpu.VMEM((group * tile_rows, HEAD), jnp.float32),
            ],
        ),
        out_shape=jax.ShapeDtypeStruct((tiles, tile_rows, cols), jnp.bfloat16),
        compiler_params=pltpu.CompilerParams(dimension_semantics=("arbitrary",)),
    )(bounds, starts, queries, *keys, *values)


def on_device(queries, keys, values, doc_lengths):
    tok_rows, q_cols = queries.shape
    kv_local = keys.shape[1] // HEAD
    group_cols = q_cols // kv_local
    half = tok_rows // 2
    cp_size = lax.axis_size("cp")
    tp_size = lax.axis_size("tp")
    me = lax.axis_index("cp")
    my_tp = lax.axis_index("tp")
    core = me % 2
    pair = me // 2
    stretch = jnp.where(core == 0, pair, cp_size - 1 - pair)
    tiles = tp_size
    tile_rows = tok_rows // tiles

    swap = [(i, i ^ 1) for i in range(cp_size)]
    ahead = [(device_of(s, cp_size), device_of(s + 1, cp_size)) for s in range(cp_size - 1)]

    def whole_stretch(array):
        mine = lax.dynamic_slice_in_dim(array, core * half, half, 0)
        other = lax.ppermute(lax.dynamic_slice_in_dim(array, (1 - core) * half, half, 0), "cp", swap)
        return jnp.concatenate([mine, other], axis=0)

    k_own = whole_stretch(keys)
    v_own = whole_stretch(values)
    q_own = whole_stretch(queries)

    ends = jnp.cumsum(doc_lengths).astype(jnp.int32)
    first_row = stretch * tok_rows
    pos = first_row + jnp.arange(tok_rows, dtype=jnp.int32)
    begin = jnp.max(jnp.where(ends[None, :] <= pos[:, None], ends[None, :], 0), axis=1)
    begin = begin - first_row + 2 * tok_rows + PAD
    starts = jnp.broadcast_to(begin[:, None], (tok_rows, 128))
    edges = begin.reshape(tiles, tile_rows)
    bounds = jnp.stack([edges[:, 0], edges[:, -1]], axis=1).reshape(-1)

    def route(k):
        pairs = []
        for c in range(cp_size):
            for t in range(tp_size):
                j = (t + k) % tiles
                dest_c = c if j < 2 else c ^ 1
                dest_t = j % 2 + 2 * (c % 2)
                pairs.append((c * tp_size + t, dest_c * tp_size + dest_t))
        return pairs

    ks, vs = [], []
    for h in range(kv_local):
        cols = slice(h * HEAD, (h + 1) * HEAD)
        k = [k_own[:, cols]]
        v = [v_own[:, cols]]
        for turn in range(2):
            k.append(lax.ppermute(k[-1], "cp", ahead))
            v.append(lax.ppermute(v[-1], "cp", ahead))
        ks.append(k)
        vs.append(v)
    received = []
    for h in range(kv_local):
        out = attend(q_own[:, h * group_cols : (h + 1) * group_cols], ks[h], vs[h], bounds, starts, tiles)
        row = []
        for k in range(tiles):
            j = (my_tp + k) % tiles
            piece = lax.dynamic_index_in_dim(out, j, 0, keepdims=False)
            row.append(lax.ppermute(piece, ("cp", "tp"), route(k)))
        received.append(row)

    result = jnp.zeros((tile_rows, tp_size * q_cols), queries.dtype)
    dest_half = my_tp // 2
    j = my_tp % 2 + 2 * jnp.where(core == dest_half, 0, 1)
    for h in range(kv_local):
        for k in range(tiles):
            source = (j - k) % tiles
            result = lax.dynamic_update_slice_in_dim(
                result, received[h][k], source * q_cols + h * group_cols, 1
            )
    return result


def solution(mesh):
    in_specs = (P("cp", "tp"), P("cp", "tp"), P("cp", "tp"), P())
    out_specs = P(("cp", "tp"), None)
    return jax.shard_map(
        on_device, mesh=mesh, in_specs=in_specs, out_specs=out_specs, check_vma=False
    )
```

```python
import functools

import jax
import jax.numpy as jnp
from jax import lax
from jax.experimental import pallas as pl
from jax.experimental.pallas import tpu as pltpu
from jax.sharding import PartitionSpec as P

HEAD = 128
TILE = 256
negative = -1e30
factor = float(HEAD) ** (-0.5) * 1.4426950408889634


anywhere = pl.BlockSpec(memory_space=pl.ANY)
scalars = pl.BlockSpec(memory_space=pltpu.SMEM)
fast = pl.BlockSpec(memory_space=pltpu.VMEM)


def device_of(stretch, cp_size):
    if stretch < cp_size // 2:
        return 2 * stretch
    return 2 * (cp_size - 1 - stretch) + 1


def run_all(copies):
    for copy in copies:
        copy.start()
    for copy in copies:
        copy.wait()


def pack_kernel(half, me, k_ref, v_ref, other_ref, sems):
    rows = pl.ds(pl.multiple_of((1 - me[0] % 2) * half, half), half)
    run_all([
        pltpu.make_async_copy(k_ref.at[rows, :], other_ref.at[0], sems.at[0]),
        pltpu.make_async_copy(v_ref.at[rows, :], other_ref.at[1], sems.at[1]),
    ])


def pack(me, keys, values):
    rows, cols = keys.shape
    half = rows // 2
    return pl.pallas_call(
        functools.partial(pack_kernel, half),
        in_specs=[scalars, anywhere, anywhere],
        out_specs=fast,
        out_shape=jax.ShapeDtypeStruct((2, half, cols), keys.dtype),
        scratch_shapes=[pltpu.SemaphoreType.DMA((2,))],
        compiler_params=pltpu.CompilerParams(vmem_limit_bytes=4 << 20),
    )(me, keys, values)


def join_kernel(half, heads, me, k_ref, v_ref, got_ref, *rest):
    outs, sems = rest[:heads], rest[heads]
    mine = pl.ds(pl.multiple_of((me[0] % 2) * half, half), half)
    copies = []
    for h in range(heads):
        cols = slice(h * HEAD, (h + 1) * HEAD)
        for n, ref in enumerate((k_ref, v_ref)):
            first = 2 * half * n
            copies.append((ref.at[mine, cols], outs[h].at[pl.ds(first, half), :]))
            copies.append((got_ref.at[n, :, cols], outs[h].at[pl.ds(first + half, half), :]))
    run_all([pltpu.make_async_copy(a, b, sems.at[i]) for i, (a, b) in enumerate(copies)])


def join(me, keys, values, got):
    rows, cols = keys.shape
    heads = cols // HEAD
    return pl.pallas_call(
        functools.partial(join_kernel, rows // 2, heads),
        in_specs=[scalars, anywhere, anywhere, fast],
        out_specs=[fast] * heads,
        out_shape=[jax.ShapeDtypeStruct((2 * rows, HEAD), keys.dtype)] * heads,
        scratch_shapes=[pltpu.SemaphoreType.DMA((4 * heads,))],
        compiler_params=pltpu.CompilerParams(vmem_limit_bytes=4 << 20),
    )(me, keys, values, got)


def attend_kernel(head, where, bounds, starts, q_ref, q_got, kv0, kv1, kv2, *rest):
    pieces = 4
    outs = rest[:pieces]
    (qbuf, kbuf, vraw, vbuf, obuf, m_ref, l_ref, keep_ref, acc_ref, s_ref, p_ref, bias_ref,
     item_t, item_k, item_m, sems) = rest[pieces:]
    rows, cols = qbuf.shape
    half = rows // 2
    tiles = rows // TILE
    group = cols // HEAD
    base = 2 * tiles

    core = where[0] % 2
    mine = pl.ds(pl.multiple_of(core * half, half), half)
    my_cols = slice(head * cols, (head + 1) * cols)
    copies = [
        (q_ref.at[mine, my_cols], qbuf.at[pl.ds(0, half), :]),
        (q_got.at[:, my_cols], qbuf.at[pl.ds(half, half), :]),
    ]
    for n, ref in enumerate((kv2, kv1, kv0)):
        copies.append((ref.at[pl.ds(0, rows), :], kbuf.at[pl.ds(n * rows, rows), :]))
        copies.append((ref.at[pl.ds(rows, rows), :], vraw.at[pl.ds(n * rows, rows), :]))
    copies = [pltpu.make_async_copy(a, b, sems.at[i]) for i, (a, b) in enumerate(copies)]
    for copy in copies:
        copy.start()

    m_ref[...] = jnp.full(m_ref.shape, negative, jnp.float32)
    l_ref[...] = jnp.zeros(l_ref.shape, jnp.float32)
    acc_ref[...] = jnp.zeros(acc_ref.shape, jnp.float32)
    keep_ref[...] = jnp.zeros(keep_ref.shape, jnp.float32)

    count = jnp.int32(0)
    for t in range(tiles):
        last_block = base + t
        first_block = bounds[2 * t] // TILE
        mask_below = (bounds[2 * t + 1] + TILE - 1) // TILE

        def add(back, c, t=t, last_block=last_block, mask_below=mask_below):
            block = last_block - back
            item_t[c] = jnp.int32(t)
            item_k[c] = block
            item_m[c] = ((block == last_block) | (block < mask_below)).astype(jnp.int32)
            return c + 1

        count = lax.fori_loop(0, last_block - first_block + 1, add, count)
    for extra in range(2):
        item_t[count + extra] = jnp.int32(tiles)
        item_k[count + extra] = jnp.int32(0)
        item_m[count + extra] = jnp.int32(0)

    for copy in copies:
        copy.wait()
    for n in range(3 * tiles):
        vbuf[n] = vraw[pl.ds(n * TILE, TILE), :].T

    def body(i, carry):
        t1, k1, t2, k2 = carry
        t = item_t[i]
        block = item_k[i]
        masked = item_m[i]

        @pl.when(masked == 1)
        def make_bias():
            key_pos = block * TILE + lax.broadcasted_iota(jnp.int32, (TILE, TILE), 0)
            own = (base + t) * TILE + lax.broadcasted_iota(jnp.int32, (TILE, TILE), 1)
            allowed = (key_pos >= starts[t]) & (key_pos <= own)
            bias_ref[...] = jnp.where(allowed, 0.0, negative)

        q_rows = pl.ds(pl.multiple_of(jnp.minimum(t, tiles - 1) * TILE, TILE), TILE)
        k_rows = pl.ds(pl.multiple_of(block * TILE, TILE), TILE)

        def stages(with_mask):
            for h in range(group):
                slot = t2 * group + h
                acc_ref[slot] = keep_ref[0, h] * acc_ref[slot] + jnp.dot(
                    vbuf[k2], p_ref[h], preferred_element_type=jnp.float32
                )
            for h in range(group):
                slot = t1 * group + h
                keep = keep_ref[1, h]
                keep_ref[0, h] = keep
                weights = jnp.exp2((s_ref[h] - m_ref[slot]) * factor)
                l_ref[slot] = keep * l_ref[slot] + jnp.sum(weights, axis=0, keepdims=True)
                p_ref[h] = weights.astype(jnp.bfloat16)
            for h in range(group):
                slot = t * group + h
                scores = lax.dot_general(
                    kbuf[k_rows, :], qbuf[q_rows, h * HEAD : (h + 1) * HEAD],
                    (((1,), (1,)), ((), ())), preferred_element_type=jnp.float32,
                )
                if with_mask:
                    scores = scores + bias_ref[...]
                s_ref[h] = scores
                old = m_ref[slot]
                new = jnp.maximum(old, jnp.max(scores, axis=0, keepdims=True))
                m_ref[slot] = new
                keep_ref[1, h] = jnp.exp2((old - new) * factor)

        @pl.when(masked == 1)
        def with_mask():
            stages(True)

        @pl.when(masked == 0)
        def without_mask():
            stages(False)

        return (t, block, t1, k1)

    zero = jnp.int32(0)
    idle = jnp.int32(tiles)
    lax.fori_loop(0, count + 2, body, (idle, zero, idle, zero))

    for t in range(tiles):
        for h in range(group):
            slot = t * group + h
            obuf[pl.ds(t * TILE, TILE), h * HEAD : (h + 1) * HEAD] = (
                (acc_ref[slot] / l_ref[slot]).astype(obuf.dtype).T
            )
    size = rows // pieces
    run_all([
        pltpu.make_async_copy(
            obuf.at[pl.ds(pl.multiple_of(((where[1] + k) % pieces) * size, size), size), :],
            outs[k], sems.at[k],
        )
        for k in range(pieces)
    ])


def attend(head, group, where, bounds, starts, queries, q_got, messages):
    rows = queries.shape[0]
    cols = group * HEAD
    tiles = rows // TILE
    slots = (tiles + 1) * group
    pieces = 4
    return pl.pallas_call(
        functools.partial(attend_kernel, head),
        in_specs=[scalars, scalars, fast, anywhere] + [fast] * 4,
        out_specs=[fast] * pieces,
        out_shape=[jax.ShapeDtypeStruct((rows // pieces, cols), queries.dtype)] * pieces,
        scratch_shapes=[
            pltpu.VMEM((rows, cols), jnp.bfloat16),
            pltpu.VMEM((3 * rows, HEAD), jnp.bfloat16),
            pltpu.VMEM((3 * rows, HEAD), jnp.bfloat16),
            pltpu.VMEM((3 * tiles, HEAD, TILE), jnp.bfloat16),
            pltpu.VMEM((rows, cols), jnp.bfloat16),
            pltpu.VMEM((slots, 1, TILE), jnp.float32),
            pltpu.VMEM((slots, 1, TILE), jnp.float32),
            pltpu.VMEM((2, group, 1, TILE), jnp.float32),
            pltpu.VMEM((slots, HEAD, TILE), jnp.float32),
            pltpu.VMEM((group, TILE, TILE), jnp.float32),
            pltpu.VMEM((group, TILE, TILE), jnp.bfloat16),
            pltpu.VMEM((TILE, TILE), jnp.float32),
            pltpu.SMEM((40,), jnp.int32),
            pltpu.SMEM((40,), jnp.int32),
            pltpu.SMEM((40,), jnp.int32),
            pltpu.SemaphoreType.DMA((8,)),
        ],
        compiler_params=pltpu.CompilerParams(vmem_limit_bytes=24 << 20),
    )(where, bounds, starts, queries, q_got, *messages)


def docs_kernel(rows, where, lengths, bounds_ref, starts_ref):
    cp_size = where[2]
    pair = where[0] // 2
    stretch = jnp.where(where[0] % 2 == 0, pair, cp_size - 1 - pair)
    origin = (stretch - 2) * rows
    tiles = rows // TILE
    pos = [
        2 * rows + t * TILE + lax.broadcasted_iota(jnp.int32, (8, TILE), 1) for t in range(tiles)
    ]

    def step(j, carry):
        end, edges, begins = carry
        end = end + lengths[j]
        edges = tuple(
            jnp.where(end <= 2 * rows + (n // 2) * TILE + (n % 2) * (TILE - 1), end, e)
            for n, e in enumerate(edges)
        )
        begins = tuple(jnp.where(p >= end, end, b) for p, b in zip(pos, begins))
        return end, edges, begins

    start = -origin
    edges = (start,) * (2 * tiles)
    begins = tuple(jnp.full((8, TILE), start, jnp.int32) for _ in range(tiles))
    _, edges, begins = lax.fori_loop(0, lengths.shape[0], step, (start, edges, begins))
    for n in range(2 * tiles):
        bounds_ref[n] = edges[n]
    for t in range(tiles):
        starts_ref[t] = begins[t][:1]


def docs(where, lengths, rows):
    tiles = rows // TILE
    return pl.pallas_call(
        functools.partial(docs_kernel, rows),
        in_specs=[scalars, scalars],
        out_specs=[scalars, fast],
        out_shape=[
            jax.ShapeDtypeStruct((2 * tiles,), jnp.int32),
            jax.ShapeDtypeStruct((tiles, 1, TILE), jnp.int32),
        ],
        compiler_params=pltpu.CompilerParams(vmem_limit_bytes=1 << 20),
    )(where, lengths)


def on_device(queries, keys, values, doc_lengths):
    tok_rows, q_cols = queries.shape
    kv_local = keys.shape[1] // HEAD
    group_cols = q_cols // kv_local
    half = tok_rows // 2
    cp_size = lax.axis_size("cp")
    tp_size = lax.axis_size("tp")
    me = lax.axis_index("cp")
    my_tp = lax.axis_index("tp")
    core = me % 2
    tile_rows = tok_rows // tp_size

    swap = [(i, i ^ 1) for i in range(cp_size)]
    ahead = [(device_of(s, cp_size), device_of(s + 1, cp_size)) for s in range(cp_size - 1)]
    where = jnp.stack([me, my_tp, jnp.int32(cp_size)]).astype(jnp.int32)

    got = lax.ppermute(pack(where, keys, values), "cp", swap)
    messages = join(where, keys, values, got)
    bounds, starts = docs(where, doc_lengths, tok_rows)
    q_got = lax.ppermute(lax.dynamic_slice_in_dim(queries, (1 - core) * half, half, 0), "cp", swap)

    def route(k):
        pairs = []
        for c in range(cp_size):
            for t in range(tp_size):
                j = (t + k) % tp_size
                dest_c = c if j < 2 else c ^ 1
                dest_t = j % 2 + 2 * (c % 2)
                pairs.append((c * tp_size + t, dest_c * tp_size + dest_t))
        return pairs

    chains = [[message] for message in messages]
    for turn in range(2):
        for chain in chains:
            chain.append(lax.ppermute(chain[-1], "cp", ahead))
    received = []
    for h in range(kv_local):
        out = attend(h, group_cols // HEAD, where, bounds, starts, queries, q_got, chains[h])
        received.append([lax.ppermute(out[k], ("cp", "tp"), route(k)) for k in range(tp_size)])

    result = jnp.zeros((tile_rows, tp_size * q_cols), queries.dtype)
    j = my_tp % 2 + 2 * jnp.where(core == my_tp // 2, 0, 1)
    for h in range(kv_local):
        for k in range(tp_size):
            source = (j - k) % tp_size
            result = lax.dynamic_update_slice_in_dim(
                result, received[h][k], source * q_cols + h * group_cols, 1
            )
    return result


def solution(mesh):
    in_specs = (P("cp", "tp"), P("cp", "tp"), P("cp", "tp"), P())
    out_specs = P(("cp", "tp"), None)
    return jax.shard_map(
        on_device, mesh=mesh, in_specs=in_specs, out_specs=out_specs, check_vma=False
    )
```

```python
import functools

import jax
import jax.numpy as jnp
from jax import lax
from jax.experimental import pallas as pl
from jax.experimental.pallas import tpu as pltpu
from jax.sharding import PartitionSpec as P


HEAD = 128
TILE = 256
negative = -1e30
factor = float(HEAD) ** (-0.5) * 1.4426950408889634


anywhere = pl.BlockSpec(memory_space=pltpu.HBM)
scalars = pl.BlockSpec(memory_space=pltpu.SMEM)
fast = pl.BlockSpec(memory_space=pltpu.VMEM)


def device_of(stretch, cp_size):
    if stretch < cp_size // 2:
        return 2 * stretch
    return 2 * (cp_size - 1 - stretch) + 1


def run_all(copies):
    for copy in copies:
        copy.start()
    for copy in copies:
        copy.wait()


def join_kernel(half, heads, bounds, k_ref, v_ref, k_got, v_got, *rest):
    del bounds
    outs, sems = rest[:heads], rest[heads]
    mine = pl.ds(pl.multiple_of((lax.axis_index("cp") % 2) * half, half), half)
    copies = []
    for h in range(heads):
        cols = slice(h * HEAD, (h + 1) * HEAD)
        for n, (own, got) in enumerate(((k_ref, k_got), (v_ref, v_got))):
            first = 2 * half * n
            copies.append((own.at[mine, cols], outs[h].at[pl.ds(first, half), :]))
            copies.append((got.at[mine, cols], outs[h].at[pl.ds(first + half, half), :]))
    run_all([pltpu.make_async_copy(a, b, sems.at[i]) for i, (a, b) in enumerate(copies)])


def join(bounds, keys, values, k_got, v_got):
    rows, cols = keys.shape
    heads = cols // HEAD
    return pl.pallas_call(
        functools.partial(join_kernel, rows // 2, heads),
        in_specs=[scalars, anywhere, anywhere, fast, fast],
        out_specs=[fast] * heads,
        out_shape=[jax.ShapeDtypeStruct((2 * rows, HEAD), keys.dtype)] * heads,
        scratch_shapes=[pltpu.SemaphoreType.DMA((4 * heads,))],
        compiler_params=pltpu.CompilerParams(vmem_limit_bytes=4 << 20),
    )(bounds, keys, values, k_got, v_got)


def attend_kernel(head, low, high, opening, closing, pieces, cp_size, far_stretches, *refs):
    refs = list(refs)
    take = lambda n: [refs.pop(0) for _ in range(n)]
    bounds, starts = take(2)
    me = lax.axis_index("cp")
    my_tp = lax.axis_index("tp")
    stretches = high // 3 - low // 3
    q_ref, q_got = take(2) if opening else (None, None)
    far = take(1)[0] if low == 0 else None
    messages = take(stretches)
    if not opening:
        take(4)
    outs = take(pieces) if closing else []
    qbuf, m_ref, l_ref, acc_ref = take(4)
    kbuf, vbuf, keep_ref, s_ref, p_ref, bias_ref, item_t, item_k, item_m = take(9)
    obuf = take(1)[0] if closing else None
    sems = take(1)[0]

    rows, cols = qbuf.shape
    half = rows // 2
    tiles = rows // TILE
    group = cols // HEAD
    base = 2 * tiles

    if opening:
        mine = pl.ds(pl.multiple_of((me % 2) * half, half), half)
        my_cols = slice(head * cols, (head + 1) * cols)
        copies = [
            pltpu.make_async_copy(q_ref.at[mine, my_cols], qbuf.at[pl.ds(0, half), :], sems.at[0]),
            pltpu.make_async_copy(q_got.at[mine, my_cols], qbuf.at[pl.ds(half, half), :], sems.at[1]),
        ]
        for copy in copies:
            copy.start()
        m_ref[...] = jnp.full(m_ref.shape, negative, jnp.float32)
        l_ref[...] = jnp.zeros(l_ref.shape, jnp.float32)
        acc_ref[...] = jnp.zeros(acc_ref.shape, jnp.float32)
    keep_ref[...] = jnp.zeros(keep_ref.shape, jnp.float32)

    count = jnp.int32(0)
    for t in range(tiles):
        last = base + t
        first_block = jnp.maximum(bounds[2 * t] // TILE, low)
        top_block = min(last, high - 1)
        mask_below = (bounds[2 * t + 1] + TILE - 1) // TILE

        def add(back, c, t=t, last=last, top_block=top_block, mask_below=mask_below):
            block = top_block - back
            item_t[c] = jnp.int32(t)
            item_k[c] = block
            item_m[c] = ((block == last) | (block < mask_below)).astype(jnp.int32)
            return c + 1

        count = lax.fori_loop(0, top_block - first_block + 1, add, count)
    for extra in range(2):
        item_t[count + extra] = jnp.int32(tiles)
        item_k[count + extra] = jnp.int32(low)
        item_m[count + extra] = jnp.int32(0)

    def load(ref, n):
        kbuf[pl.ds(n * rows, rows), :] = ref[pl.ds(0, rows), :]
        for i in range(tiles):
            vbuf[n * tiles + i] = ref[pl.ds(rows + i * TILE, TILE), :].T

    def load_all():
        for n, ref in enumerate(messages):
            if n == 0 and far is not None:
                stretch = stretch_of(me, cp_size)
                is_far = functools.reduce(jnp.logical_or, [stretch == s for s in far_stretches])

                @pl.when(is_far)
                def from_far():
                    load(far, 0)

                @pl.when(jnp.logical_not(is_far))
                def from_near(ref=ref):
                    load(ref, 0)
            else:
                load(ref, n)

    def body(i, carry):
        t1, k1, t2, k2 = carry
        t = item_t[i]
        block = item_k[i]
        masked = item_m[i]

        @pl.when(masked == 1)
        def make_bias():
            key_pos = block * TILE + lax.broadcasted_iota(jnp.int32, (TILE, TILE), 0)
            own = (base + t) * TILE + lax.broadcasted_iota(jnp.int32, (TILE, TILE), 1)
            allowed = (key_pos >= starts[t]) & (key_pos <= own)
            bias_ref[...] = jnp.where(allowed, 0.0, negative)

        q_rows = pl.ds(pl.multiple_of(jnp.minimum(t, tiles - 1) * TILE, TILE), TILE)
        k_rows = pl.ds(pl.multiple_of((block - low) * TILE, TILE), TILE)

        def stages(with_mask):
            for h in range(group):
                slot = t2 * group + h
                acc_ref[slot] = keep_ref[0, h] * acc_ref[slot] + jnp.dot(
                    vbuf[k2 - low], p_ref[h], preferred_element_type=jnp.float32
                )
            for h in range(group):
                slot = t1 * group + h
                keep = keep_ref[1, h]
                keep_ref[0, h] = keep
                weights = jnp.exp2((s_ref[h] - m_ref[slot]) * factor)
                l_ref[slot] = keep * l_ref[slot] + jnp.sum(weights, axis=0, keepdims=True)
                p_ref[h] = weights.astype(jnp.bfloat16)
            for h in range(group):
                slot = t * group + h
                scores = lax.dot_general(
                    kbuf[k_rows, :], qbuf[q_rows, h * HEAD : (h + 1) * HEAD],
                    (((1,), (1,)), ((), ())), preferred_element_type=jnp.float32,
                )
                if with_mask:
                    scores = scores + bias_ref[...]
                s_ref[h] = scores
                old = m_ref[slot]
                new = jnp.maximum(old, jnp.max(scores, axis=0, keepdims=True))
                m_ref[slot] = new
                keep_ref[1, h] = jnp.exp2((old - new) * factor)

        @pl.when(masked == 1)
        def with_mask():
            stages(True)

        @pl.when(masked == 0)
        def without_mask():
            stages(False)

        return (t, block, t1, k1)

    def run():
        load_all()
        start = (jnp.int32(tiles), jnp.int32(low)) * 2
        lax.fori_loop(0, count + 2, body, start)

    if opening:
        for copy in copies:
            copy.wait()
        run()
    else:
        pl.when(count > 0)(run)

    if closing:
        for t in range(tiles):
            for h in range(group):
                slot = t * group + h
                obuf[pl.ds(t * TILE, TILE), h * HEAD : (h + 1) * HEAD] = (
                    (acc_ref[slot] / l_ref[slot]).astype(obuf.dtype).T
                )
        size = rows // pieces
        run_all([
            pltpu.make_async_copy(
                obuf.at[pl.ds(pl.multiple_of(((my_tp + k) % pieces) * size, size), size), :],
                outs[k], sems.at[k],
            )
            for k in range(pieces)
        ])


def attend(head, low, group, pieces, cp_size, far_stretches, bounds, starts, q_pair, messages, state=None, closing=True):
    opening = state is None
    rows = messages[0].shape[0] // 2
    cols = group * HEAD
    tiles = rows // TILE
    stretches = len(messages) - (low == 0)
    high = low + stretches * tiles
    slots = (tiles + 1) * group
    held = [
        ((rows, cols), jnp.bfloat16),
        ((slots, 1, TILE), jnp.float32),
        ((slots, 1, TILE), jnp.float32),
        ((slots, HEAD, TILE), jnp.float32),
    ]
    scratch = [
        pltpu.VMEM((stretches * rows, HEAD), jnp.bfloat16),
        pltpu.VMEM((stretches * tiles, HEAD, TILE), jnp.bfloat16),
        pltpu.VMEM((2, group, 1, TILE), jnp.float32),
        pltpu.VMEM((group, TILE, TILE), jnp.float32),
        pltpu.VMEM((group, TILE, TILE), jnp.bfloat16),
        pltpu.VMEM((TILE, TILE), jnp.float32),
        pltpu.SMEM((40,), jnp.int32),
        pltpu.SMEM((40,), jnp.int32),
        pltpu.SMEM((40,), jnp.int32),
    ]
    outs = []
    if closing:
        scratch.append(pltpu.VMEM((rows, cols), jnp.bfloat16))
        outs = [jax.ShapeDtypeStruct((rows // pieces, cols), jnp.bfloat16)] * pieces
    scratch.append(pltpu.SemaphoreType.DMA((8,)))
    operands = [bounds, starts]
    specs = [scalars, fast]
    if opening:
        operands += list(q_pair)
        specs += [anywhere, fast]
    operands += messages
    specs += [fast] * len(messages)
    aliases = {}
    if opening and closing:
        scratch = [pltpu.VMEM(*h) for h in held] + scratch
    else:
        if not opening:
            for n in range(len(held)):
                aliases[len(operands) + n] = len(outs) + n
            operands += state
            specs += [fast] * len(held)
        outs = outs + [jax.ShapeDtypeStruct(*h) for h in held]
    return pl.pallas_call(
        functools.partial(
            attend_kernel, head, low, high, opening, closing, pieces, cp_size, far_stretches
        ),
        in_specs=specs,
        out_specs=[fast] * len(outs),
        out_shape=outs,
        scratch_shapes=scratch,
        input_output_aliases=aliases,
        compiler_params=pltpu.CompilerParams(vmem_limit_bytes=12 << 20),
    )(*operands)


def stretch_of(device, cp_size):
    return jnp.where(device % 2 == 0, device // 2, cp_size - 1 - device // 2)


def docs_kernel(rows, cp_size, lengths, bounds_ref, starts_ref):
    stretch = stretch_of(lax.axis_index("cp"), cp_size)
    origin = (stretch - 2) * rows
    tiles = rows // TILE
    pos = [
        2 * rows + t * TILE + lax.broadcasted_iota(jnp.int32, (8, TILE), 1) for t in range(tiles)
    ]

    def step(j, carry):
        end, edges, begins = carry
        end = end + lengths[j]
        edges = tuple(
            jnp.where(end <= 2 * rows + (n // 2) * TILE + (n % 2) * (TILE - 1), end, e)
            for n, e in enumerate(edges)
        )
        begins = tuple(jnp.where(p >= end, end, b) for p, b in zip(pos, begins))
        return end, edges, begins

    start = -origin
    edges = (start,) * (2 * tiles)
    begins = tuple(jnp.full((8, TILE), start, jnp.int32) for _ in range(tiles))
    _, edges, begins = lax.fori_loop(0, lengths.shape[0], step, (start, edges, begins))
    for n in range(2 * tiles):
        bounds_ref[n] = edges[n]
    for t in range(tiles):
        starts_ref[t] = begins[t][:1]


def docs(lengths, rows, cp_size):
    tiles = rows // TILE
    return pl.pallas_call(
        functools.partial(docs_kernel, rows, cp_size),
        in_specs=[scalars],
        out_specs=[scalars, fast],
        out_shape=[
            jax.ShapeDtypeStruct((2 * tiles,), jnp.int32),
            jax.ShapeDtypeStruct((tiles, 1, TILE), jnp.int32),
        ],
        compiler_params=pltpu.CompilerParams(vmem_limit_bytes=1 << 20),
    )(lengths)


def place_kernel(head, heads, *refs):
    pieces = len(refs) - 2 - (head > 0)
    out, sems = refs[-2:]
    _, cols = refs[0].shape
    t = lax.axis_index("tp")
    j = t % 2 + 2 * jnp.where(lax.axis_index("cp") % 2 == t // 2, 0, 1)
    run_all([
        pltpu.make_async_copy(
            refs[k],
            out.at[:, pl.ds(pl.multiple_of(((j + pieces - k) % pieces) * (heads * cols) + head * cols, cols), cols)],
            sems.at[k],
        )
        for k in range(pieces)
    ])


def place(head, heads, pieces, result):
    rows, cols = pieces[0].shape
    operands = [*pieces] + ([] if result is None else [result])
    return pl.pallas_call(
        functools.partial(place_kernel, head, heads),
        in_specs=[fast] * len(pieces) + [anywhere] * (result is not None),
        out_specs=anywhere,
        out_shape=jax.ShapeDtypeStruct((rows, cols * heads * len(pieces)), pieces[0].dtype),
        scratch_shapes=[pltpu.SemaphoreType.DMA((len(pieces),))],
        input_output_aliases={} if result is None else {len(operands) - 1: 0},
        compiler_params=pltpu.CompilerParams(vmem_limit_bytes=4 << 20),
    )(*operands)


def on_device(queries, keys, values, doc_lengths):
    tok_rows, q_cols = queries.shape
    kv_local = keys.shape[1] // HEAD
    group_cols = q_cols // kv_local
    cp_size = lax.axis_size("cp")
    tp_size = lax.axis_size("tp")

    swap = [(i, i ^ 1) for i in range(cp_size)]
    link = lambda s, d: (device_of(s, cp_size), device_of(s + d, cp_size))
    ahead = [link(s, 1) for s in range(cp_size - 1)]
    long_hops = [cp_size // 4 - 1, cp_size - 1 - cp_size // 4]
    handed = [link(s, 1) for s in range(cp_size - 1) if s not in long_hops]
    direct = [link(s - 1, 2) for s in long_hops]
    far_stretches = [s + 1 for s in long_hops]

    def route(k):
        pairs = []
        for c in range(cp_size):
            for t in range(tp_size):
                j = (t + k) % tp_size
                dest_c = c if j < 2 else c ^ 1
                dest_t = j % 2 + 2 * (c % 2)
                pairs.append((c * tp_size + t, dest_c * tp_size + dest_t))
        return pairs

    k_got = lax.ppermute(keys, "cp", swap)
    v_got = lax.ppermute(values, "cp", swap)
    q_got = lax.ppermute(queries, "cp", swap)
    bounds, starts = docs(doc_lengths, tok_rows, cp_size)
    messages = join(bounds, keys, values, k_got, v_got)

    near = [lax.ppermute(messages[h], "cp", ahead) for h in range(kv_local)]
    far = [lax.ppermute(messages[h], "cp", direct) for h in range(kv_local)]
    next_near = [lax.ppermute(near[h], "cp", handed) for h in range(kv_local)]
    group = group_cols // HEAD
    tiles = tok_rows // TILE
    q_pair = (queries, q_got)
    received = []
    for h in range(kv_local):
        if h == 0:
            state = attend(h, tiles, group, tp_size, cp_size, far_stretches, bounds, starts, q_pair,
                          [near[h], messages[h]], closing=False)
            out = attend(h, 0, group, tp_size, cp_size, far_stretches, bounds, starts, q_pair,
                        [far[h], next_near[h]], state=state)
        else:
            out = attend(h, 0, group, tp_size, cp_size, far_stretches, bounds, starts, q_pair,
                        [far[h], next_near[h], near[h], messages[h]])
        received.append([lax.ppermute(out[k], ("cp", "tp"), route(k)) for k in range(tp_size)])

    result = None
    for h in range(kv_local):
        result = place(h, kv_local, received[h], result)
    return result


def solution(mesh):
    in_specs = (P("cp", "tp"), P("cp", "tp"), P("cp", "tp"), P())
    out_specs = P(("cp", "tp"), None)
    return jax.shard_map(on_device, mesh=mesh, in_specs=in_specs, out_specs=out_specs, check_vma=False)
```

```python
import functools

import jax
import jax.numpy as jnp
from jax import lax
from jax.experimental import pallas as pl
from jax.experimental.pallas import tpu as pltpu
from jax.sharding import PartitionSpec as P


HEAD = 128
TILE = 256
negative = -1e30
factor = float(HEAD) ** (-0.5) * 1.4426950408889634


anywhere = pl.BlockSpec(memory_space=pltpu.HBM)
scalars = pl.BlockSpec(memory_space=pltpu.SMEM)
fast = pl.BlockSpec(memory_space=pltpu.VMEM)


def device_of(stretch, cp_size):
    if stretch < cp_size // 2:
        return 2 * stretch
    return 2 * (cp_size - 1 - stretch) + 1


def run_all(copies):
    for copy in copies:
        copy.start()
    for copy in copies:
        copy.wait()


def join_kernel(half, heads, k_ref, v_ref, k_got, v_got, *rest):
    outs, every, sems = rest[:heads], rest[heads], rest[heads + 1]
    mine = pl.ds(pl.multiple_of((lax.axis_index("cp") % 2) * half, half), half)
    copies = []
    for h in range(heads):
        cols = slice(h * HEAD, (h + 1) * HEAD)
        for n, (own, got) in enumerate(((k_ref, k_got), (v_ref, v_got))):
            for out, skip in ((outs[h], 0), (every, 4 * half * h)):
                first = skip + 2 * half * n
                copies.append((own.at[mine, cols], out.at[pl.ds(first, half), :]))
                copies.append((got.at[mine, cols], out.at[pl.ds(first + half, half), :]))
    run_all([pltpu.make_async_copy(a, b, sems.at[i]) for i, (a, b) in enumerate(copies)])


def join(keys, values, k_got, v_got):
    rows, cols = keys.shape
    heads = cols // HEAD
    return pl.pallas_call(
        functools.partial(join_kernel, rows // 2, heads),
        in_specs=[anywhere, anywhere, fast, fast],
        out_specs=[fast] * (heads + 1),
        out_shape=[jax.ShapeDtypeStruct((2 * rows, HEAD), keys.dtype)] * heads
        + [jax.ShapeDtypeStruct((2 * rows * heads, HEAD), keys.dtype)],
        scratch_shapes=[pltpu.SemaphoreType.DMA((8 * heads,))],
        compiler_params=pltpu.CompilerParams(vmem_limit_bytes=4 << 20),
    )(keys, values, k_got, v_got)


def attend_kernel(head, low, high, opening, closing, pieces, cp_size, far_stretches, *refs):
    refs = list(refs)
    take = lambda n: [refs.pop(0) for _ in range(n)]
    bounds, starts = take(2)
    me = lax.axis_index("cp")
    my_tp = lax.axis_index("tp")
    stretches = high // 3 - low // 3
    q_ref, q_got = take(2) if opening else (None, None)
    far = take(1)[0] if low == 0 else None
    messages = take(stretches)
    if not opening:
        take(4)
    outs = take(pieces) if closing else []
    qbuf, m_ref, l_ref, acc_ref = take(4)
    kbuf, vbuf, keep_ref, s_ref, p_ref, bias_ref, item_t, item_k, item_m = take(9)
    obuf = take(1)[0] if closing else None
    sems = take(1)[0]

    rows, cols = qbuf.shape
    half = rows // 2
    tiles = rows // TILE
    group = cols // HEAD
    base = 2 * tiles

    if opening:
        mine = pl.ds(pl.multiple_of((me % 2) * half, half), half)
        my_cols = slice(head * cols, (head + 1) * cols)
        copies = [
            pltpu.make_async_copy(q_ref.at[mine, my_cols], qbuf.at[pl.ds(0, half), :], sems.at[0]),
            pltpu.make_async_copy(q_got.at[mine, my_cols], qbuf.at[pl.ds(half, half), :], sems.at[1]),
        ]
        for copy in copies:
            copy.start()
        m_ref[...] = jnp.full(m_ref.shape, negative, jnp.float32)
        l_ref[...] = jnp.zeros(l_ref.shape, jnp.float32)
        acc_ref[...] = jnp.zeros(acc_ref.shape, jnp.float32)
    keep_ref[...] = jnp.zeros(keep_ref.shape, jnp.float32)

    count = jnp.int32(0)
    for t in range(tiles):
        last = base + t
        first_block = jnp.maximum(bounds[2 * t] // TILE, low)
        top_block = min(last, high - 1)
        mask_below = (bounds[2 * t + 1] + TILE - 1) // TILE

        def add(back, c, t=t, last=last, top_block=top_block, mask_below=mask_below):
            block = top_block - back
            item_t[c] = jnp.int32(t)
            item_k[c] = block
            item_m[c] = ((block == last) | (block < mask_below)).astype(jnp.int32)
            return c + 1

        count = lax.fori_loop(0, top_block - first_block + 1, add, count)
    for extra in range(2):
        item_t[count + extra] = jnp.int32(tiles)
        item_k[count + extra] = jnp.int32(low)
        item_m[count + extra] = jnp.int32(0)

    def load(ref, n, skip=0):
        kbuf[pl.ds(n * rows, rows), :] = ref[pl.ds(skip, rows), :]
        for i in range(tiles):
            vbuf[n * tiles + i] = ref[pl.ds(skip + rows + i * TILE, TILE), :].T

    def load_all():
        for n, ref in enumerate(messages):
            if n == 0 and far is not None:
                stretch = stretch_of(me, cp_size)
                is_far = functools.reduce(jnp.logical_or, [stretch == s for s in far_stretches])

                @pl.when(is_far)
                def from_far():
                    load(far, 0, 2 * rows * head)

                @pl.when(jnp.logical_not(is_far))
                def from_near(ref=ref):
                    load(ref, 0)
            else:
                load(ref, n)

    def body(i, carry):
        t1, k1, t2, k2 = carry
        t = item_t[i]
        block = item_k[i]
        masked = item_m[i]

        @pl.when(masked == 1)
        def make_bias():
            key_pos = block * TILE + lax.broadcasted_iota(jnp.int32, (TILE, TILE), 0)
            own = (base + t) * TILE + lax.broadcasted_iota(jnp.int32, (TILE, TILE), 1)
            allowed = (key_pos >= starts[t]) & (key_pos <= own)
            bias_ref[...] = jnp.where(allowed, 0.0, negative)

        q_rows = pl.ds(pl.multiple_of(jnp.minimum(t, tiles - 1) * TILE, TILE), TILE)
        k_rows = pl.ds(pl.multiple_of((block - low) * TILE, TILE), TILE)

        def stages(with_mask):
            for h in range(group):
                slot = t2 * group + h
                acc_ref[slot] = keep_ref[0, h] * acc_ref[slot] + jnp.dot(
                    vbuf[k2 - low], p_ref[h], preferred_element_type=jnp.float32
                )
            for h in range(group):
                slot = t1 * group + h
                keep = keep_ref[1, h]
                keep_ref[0, h] = keep
                weights = jnp.exp2((s_ref[h] - m_ref[slot]) * factor)
                l_ref[slot] = keep * l_ref[slot] + jnp.sum(weights, axis=0, keepdims=True)
                p_ref[h] = weights.astype(jnp.bfloat16)
            for h in range(group):
                slot = t * group + h
                scores = lax.dot_general(
                    kbuf[k_rows, :], qbuf[q_rows, h * HEAD : (h + 1) * HEAD],
                    (((1,), (1,)), ((), ())), preferred_element_type=jnp.float32,
                )
                if with_mask:
                    scores = scores + bias_ref[...]
                s_ref[h] = scores
                old = m_ref[slot]
                new = jnp.maximum(old, jnp.max(scores, axis=0, keepdims=True))
                m_ref[slot] = new
                keep_ref[1, h] = jnp.exp2((old - new) * factor)

        @pl.when(masked == 1)
        def with_mask():
            stages(True)

        @pl.when(masked == 0)
        def without_mask():
            stages(False)

        return (t, block, t1, k1)

    def run():
        load_all()
        start = (jnp.int32(tiles), jnp.int32(low)) * 2
        lax.fori_loop(0, count + 2, body, start)

    if opening:
        for copy in copies:
            copy.wait()
        run()
    else:
        pl.when(count > 0)(run)

    if closing:
        for t in range(tiles):
            for h in range(group):
                slot = t * group + h
                obuf[pl.ds(t * TILE, TILE), h * HEAD : (h + 1) * HEAD] = (
                    (acc_ref[slot] / l_ref[slot]).astype(obuf.dtype).T
                )
        size = rows // pieces
        run_all([
            pltpu.make_async_copy(
                obuf.at[pl.ds(pl.multiple_of(((my_tp + k) % pieces) * size, size), size), :],
                outs[k], sems.at[k],
            )
            for k in range(pieces)
        ])


def attend(head, low, group, pieces, cp_size, far_stretches, bounds, starts, q_pair, messages, state=None, closing=True):
    opening = state is None
    rows = messages[-1].shape[0] // 2
    cols = group * HEAD
    tiles = rows // TILE
    stretches = len(messages) - (low == 0)
    high = low + stretches * tiles
    slots = (tiles + 1) * group
    held = [
        ((rows, cols), jnp.bfloat16),
        ((slots, 1, TILE), jnp.float32),
        ((slots, 1, TILE), jnp.float32),
        ((slots, HEAD, TILE), jnp.float32),
    ]
    scratch = [
        pltpu.VMEM((stretches * rows, HEAD), jnp.bfloat16),
        pltpu.VMEM((stretches * tiles, HEAD, TILE), jnp.bfloat16),
        pltpu.VMEM((2, group, 1, TILE), jnp.float32),
        pltpu.VMEM((group, TILE, TILE), jnp.float32),
        pltpu.VMEM((group, TILE, TILE), jnp.bfloat16),
        pltpu.VMEM((TILE, TILE), jnp.float32),
        pltpu.SMEM((40,), jnp.int32),
        pltpu.SMEM((40,), jnp.int32),
        pltpu.SMEM((40,), jnp.int32),
    ]
    outs = []
    if closing:
        scratch.append(pltpu.VMEM((rows, cols), jnp.bfloat16))
        outs = [jax.ShapeDtypeStruct((rows // pieces, cols), jnp.bfloat16)] * pieces
    scratch.append(pltpu.SemaphoreType.DMA((8,)))
    operands = [bounds, starts]
    specs = [scalars, fast]
    if opening:
        operands += list(q_pair)
        specs += [anywhere, fast]
    operands += messages
    specs += [fast] * len(messages)
    aliases = {}
    if opening and closing:
        scratch = [pltpu.VMEM(*h) for h in held] + scratch
    else:
        if not opening:
            for n in range(len(held)):
                aliases[len(operands) + n] = len(outs) + n
            operands += state
            specs += [fast] * len(held)
        outs = outs + [jax.ShapeDtypeStruct(*h) for h in held]
    return pl.pallas_call(
        functools.partial(
            attend_kernel, head, low, high, opening, closing, pieces, cp_size, far_stretches
        ),
        in_specs=specs,
        out_specs=[fast] * len(outs),
        out_shape=outs,
        scratch_shapes=scratch,
        input_output_aliases=aliases,
        compiler_params=pltpu.CompilerParams(vmem_limit_bytes=12 << 20),
    )(*operands)


def stretch_of(device, cp_size):
    return jnp.where(device % 2 == 0, device // 2, cp_size - 1 - device // 2)


def docs_kernel(rows, cp_size, lengths, bounds_ref, starts_ref):
    stretch = stretch_of(lax.axis_index("cp"), cp_size)
    origin = (stretch - 2) * rows
    tiles = rows // TILE
    pos = [
        2 * rows + t * TILE + lax.broadcasted_iota(jnp.int32, (8, TILE), 1) for t in range(tiles)
    ]

    def step(j, carry):
        end, edges, begins = carry
        end = end + lengths[j]
        edges = tuple(
            jnp.where(end <= 2 * rows + (n // 2) * TILE + (n % 2) * (TILE - 1), end, e)
            for n, e in enumerate(edges)
        )
        begins = tuple(jnp.where(p >= end, end, b) for p, b in zip(pos, begins))
        return end, edges, begins

    start = -origin
    edges = (start,) * (2 * tiles)
    begins = tuple(jnp.full((8, TILE), start, jnp.int32) for _ in range(tiles))
    _, edges, begins = lax.fori_loop(0, lengths.shape[0], step, (start, edges, begins))
    for n in range(2 * tiles):
        bounds_ref[n] = edges[n]
    for t in range(tiles):
        starts_ref[t] = begins[t][:1]


def docs(lengths, rows, cp_size):
    tiles = rows // TILE
    return pl.pallas_call(
        functools.partial(docs_kernel, rows, cp_size),
        in_specs=[scalars],
        out_specs=[scalars, fast],
        out_shape=[
            jax.ShapeDtypeStruct((2 * tiles,), jnp.int32),
            jax.ShapeDtypeStruct((tiles, 1, TILE), jnp.int32),
        ],
        compiler_params=pltpu.CompilerParams(vmem_limit_bytes=1 << 20),
    )(lengths)


def place_kernel(head, heads, *refs):
    pieces = len(refs) - 2 - (head > 0)
    out, sems = refs[-2:]
    _, cols = refs[0].shape
    t = lax.axis_index("tp")
    j = t % 2 + 2 * jnp.where(lax.axis_index("cp") % 2 == t // 2, 0, 1)
    run_all([
        pltpu.make_async_copy(
            refs[k],
            out.at[:, pl.ds(pl.multiple_of(((j + pieces - k) % pieces) * (heads * cols) + head * cols, cols), cols)],
            sems.at[k],
        )
        for k in range(pieces)
    ])


def place(head, heads, pieces, result):
    rows, cols = pieces[0].shape
    operands = [*pieces] + ([] if result is None else [result])
    return pl.pallas_call(
        functools.partial(place_kernel, head, heads),
        in_specs=[fast] * len(pieces) + [anywhere] * (result is not None),
        out_specs=anywhere,
        out_shape=jax.ShapeDtypeStruct((rows, cols * heads * len(pieces)), pieces[0].dtype),
        scratch_shapes=[pltpu.SemaphoreType.DMA((len(pieces),))],
        input_output_aliases={} if result is None else {len(operands) - 1: 0},
        compiler_params=pltpu.CompilerParams(vmem_limit_bytes=4 << 20),
    )(*operands)


def on_device(queries, keys, values, doc_lengths):
    tok_rows, q_cols = queries.shape
    kv_local = keys.shape[1] // HEAD
    group_cols = q_cols // kv_local
    cp_size = lax.axis_size("cp")
    tp_size = lax.axis_size("tp")

    swap = [(i, i ^ 1) for i in range(cp_size)]
    link = lambda s, d: (device_of(s, cp_size), device_of(s + d, cp_size))
    ahead = [link(s, 1) for s in range(cp_size - 1)]
    long_hops = [cp_size // 4 - 1, cp_size - 1 - cp_size // 4]
    handed = [link(s, 1) for s in range(cp_size - 1) if s not in long_hops]
    direct = [link(s - 1, 2) for s in long_hops]
    far_stretches = [s + 1 for s in long_hops]

    def route(k):
        pairs = []
        for c in range(cp_size):
            for t in range(tp_size):
                j = (t + k) % tp_size
                dest_c = c if j < 2 else c ^ 1
                dest_t = j % 2 + 2 * (c % 2)
                pairs.append((c * tp_size + t, dest_c * tp_size + dest_t))
        return pairs

    k_got = lax.ppermute(keys, "cp", swap)
    v_got = lax.ppermute(values, "cp", swap)
    q_got = lax.ppermute(queries, "cp", swap)
    bounds, starts = docs(doc_lengths, tok_rows, cp_size)
    *messages, every = join(keys, values, k_got, v_got)

    near = [lax.ppermute(messages[h], "cp", ahead) for h in range(kv_local)]
    far = lax.ppermute(every, "cp", direct)
    next_near = [lax.ppermute(near[h], "cp", handed) for h in range(kv_local)]
    group = group_cols // HEAD
    tiles = tok_rows // TILE
    q_pair = (queries, q_got)
    received = []
    for h in range(kv_local):
        if h == 0:
            state = attend(h, tiles, group, tp_size, cp_size, far_stretches, bounds, starts, q_pair,
                          [near[h], messages[h]], closing=False)
            out = attend(h, 0, group, tp_size, cp_size, far_stretches, bounds, starts, q_pair,
                        [far, next_near[h]], state=state)
        else:
            out = attend(h, 0, group, tp_size, cp_size, far_stretches, bounds, starts, q_pair,
                        [far, next_near[h], near[h], messages[h]])
        received.append([lax.ppermute(out[k], ("cp", "tp"), route(k)) for k in range(tp_size)])

    result = None
    for h in range(kv_local):
        result = place(h, kv_local, received[h], result)
    return result


def solution(mesh):
    in_specs = (P("cp", "tp"), P("cp", "tp"), P("cp", "tp"), P())
    out_specs = P(("cp", "tp"), None)
    return jax.shard_map(on_device, mesh=mesh, in_specs=in_specs, out_specs=out_specs, check_vma=False)
```

```python
import functools

import jax
import jax.numpy as jnp
from jax import lax
from jax.experimental import pallas as pl
from jax.experimental.pallas import tpu as pltpu
from jax.sharding import PartitionSpec as P


HEAD = 128
TILE = 256
negative = -1e30
factor = float(HEAD) ** (-0.5) * 1.4426950408889634


anywhere = pl.BlockSpec(memory_space=pltpu.HBM)
scalars = pl.BlockSpec(memory_space=pltpu.SMEM)
fast = pl.BlockSpec(memory_space=pltpu.VMEM)


def device_of(stretch, cp_size):
    if stretch < cp_size // 2:
        return 2 * stretch
    return 2 * (cp_size - 1 - stretch) + 1


def run_all(copies):
    for copy in copies:
        copy.start()
    for copy in copies:
        copy.wait()


def join_kernel(half, heads, k_ref, v_ref, k_got, v_got, bounds, *rest):
    del bounds
    outs, sems = rest[:heads], rest[heads]
    mine = pl.ds(pl.multiple_of((lax.axis_index("cp") % 2) * half, half), half)
    copies = []
    for h in range(heads):
        cols = slice(h * HEAD, (h + 1) * HEAD)
        for n, (own, got) in enumerate(((k_ref, k_got), (v_ref, v_got))):
            first = 2 * half * n
            copies.append((own.at[mine, cols], outs[h].at[pl.ds(first, half), :]))
            copies.append((got.at[mine, cols], outs[h].at[pl.ds(first + half, half), :]))
    run_all([pltpu.make_async_copy(a, b, sems.at[i]) for i, (a, b) in enumerate(copies)])


def join(keys, values, k_got, v_got, bounds):
    rows, cols = keys.shape
    heads = cols // HEAD
    return pl.pallas_call(
        functools.partial(join_kernel, rows // 2, heads),
        in_specs=[anywhere, anywhere, fast, fast, scalars],
        out_specs=[fast] * heads,
        out_shape=[jax.ShapeDtypeStruct((2 * rows, HEAD), keys.dtype)] * heads,
        scratch_shapes=[pltpu.SemaphoreType.DMA((4 * heads,))],
        compiler_params=pltpu.CompilerParams(vmem_limit_bytes=4 << 20),
    )(keys, values, k_got, v_got, bounds)


def attend_kernel(head, low, high, opening, closing, pieces, cp_size, far_stretches, *refs):
    refs = list(refs)
    take = lambda n: [refs.pop(0) for _ in range(n)]
    bounds, starts = take(2)
    me = lax.axis_index("cp")
    my_tp = lax.axis_index("tp")
    stretches = high // 3 - low // 3
    q_ref, q_got = take(2) if opening else (None, None)
    far = take(1)[0] if low == 0 else None
    messages = take(stretches)
    if not opening:
        take(4)
    outs = take(pieces) if closing else []
    qbuf, m_ref, l_ref, acc_ref = take(4)
    kbuf, vbuf, keep_ref, s_ref, p_ref, bias_ref, item_t, item_k, item_m = take(9)
    obuf = take(1)[0] if closing else None
    sems = take(1)[0]

    rows, cols = qbuf.shape
    half = rows // 2
    tiles = rows // TILE
    group = cols // HEAD
    base = 2 * tiles

    if opening:
        mine = pl.ds(pl.multiple_of((me % 2) * half, half), half)
        my_cols = slice(head * cols, (head + 1) * cols)
        copies = [
            pltpu.make_async_copy(q_ref.at[mine, my_cols], qbuf.at[pl.ds(0, half), :], sems.at[0]),
            pltpu.make_async_copy(q_got.at[mine, my_cols], qbuf.at[pl.ds(half, half), :], sems.at[1]),
        ]
        for copy in copies:
            copy.start()
        m_ref[...] = jnp.full(m_ref.shape, negative, jnp.float32)
        l_ref[...] = jnp.zeros(l_ref.shape, jnp.float32)
        acc_ref[...] = jnp.zeros(acc_ref.shape, jnp.float32)
    keep_ref[...] = jnp.zeros(keep_ref.shape, jnp.float32)

    count = jnp.int32(0)
    for t in range(tiles):
        last = base + t
        first_block = jnp.maximum(bounds[2 * t] // TILE, low)
        top_block = min(last, high - 1)
        mask_below = (bounds[2 * t + 1] + TILE - 1) // TILE

        def add(back, c, t=t, last=last, top_block=top_block, mask_below=mask_below):
            block = top_block - back
            item_t[c] = jnp.int32(t)
            item_k[c] = block
            item_m[c] = ((block == last) | (block < mask_below)).astype(jnp.int32)
            return c + 1

        count = lax.fori_loop(0, top_block - first_block + 1, add, count)

    def load(ref, n):
        kbuf[pl.ds(n * rows, rows), :] = ref[pl.ds(0, rows), :]
        for i in range(tiles):
            vbuf[n * tiles + i] = ref[pl.ds(rows + i * TILE, TILE), :].T

    def load_all():
        for n, ref in enumerate(messages):
            if n == 0 and far is not None:
                stretch = stretch_of(me, cp_size)
                is_far = functools.reduce(jnp.logical_or, [stretch == s for s in far_stretches])

                @pl.when(is_far)
                def from_far():
                    load(far, 0)

                @pl.when(jnp.logical_not(is_far))
                def from_near(ref=ref):
                    load(ref, 0)
            else:
                load(ref, n)

    def output_stage(t, block):
        for h in range(group):
            slot = t * group + h
            acc_ref[slot] = keep_ref[0, h] * acc_ref[slot] + jnp.dot(
                vbuf[block - low], p_ref[h], preferred_element_type=jnp.float32
            )

    def weight_stage(t):
        for h in range(group):
            slot = t * group + h
            keep = keep_ref[1, h]
            keep_ref[0, h] = keep
            weights = jnp.exp2((s_ref[h] - m_ref[slot]) * factor)
            l_ref[slot] = keep * l_ref[slot] + jnp.sum(weights, axis=0, keepdims=True)
            p_ref[h] = weights.astype(jnp.bfloat16)

    def score_stage(t, block, with_mask):
        q_rows = pl.ds(pl.multiple_of(t * TILE, TILE), TILE)
        k_rows = pl.ds(pl.multiple_of((block - low) * TILE, TILE), TILE)
        for h in range(group):
            slot = t * group + h
            scores = lax.dot_general(
                kbuf[k_rows, :], qbuf[q_rows, h * HEAD : (h + 1) * HEAD],
                (((1,), (1,)), ((), ())), preferred_element_type=jnp.float32,
            )
            if with_mask:
                scores = scores + bias_ref[...]
            s_ref[h] = scores
            old = m_ref[slot]
            new = jnp.maximum(old, jnp.max(scores, axis=0, keepdims=True))
            m_ref[slot] = new
            keep_ref[1, h] = jnp.exp2((old - new) * factor)

    def with_item(i, before):
        t = item_t[i]
        block = item_k[i]
        masked = item_m[i]

        @pl.when(masked == 1)
        def with_mask():
            key_pos = block * TILE + lax.broadcasted_iota(jnp.int32, (TILE, TILE), 0)
            own = (base + t) * TILE + lax.broadcasted_iota(jnp.int32, (TILE, TILE), 1)
            allowed = (key_pos >= starts[t]) & (key_pos <= own)
            bias_ref[...] = jnp.where(allowed, 0.0, negative)
            before()
            score_stage(t, block, True)

        @pl.when(masked == 0)
        def without_mask():
            before()
            score_stage(t, block, False)

        return t, block

    def body(i, carry):
        t1, k1, t2, k2 = carry

        def before():
            output_stage(t2, k2)
            weight_stage(t1)

        return (*with_item(i, before), t1, k1)

    def run():
        load_all()
        first = with_item(0, lambda: None)
        t1, k1, t2, k2 = lax.fori_loop(1, count, body, (*first, jnp.int32(tiles), jnp.int32(low)))
        output_stage(t2, k2)
        weight_stage(t1)
        output_stage(t1, k1)

    if opening:
        for copy in copies:
            copy.wait()
        run()
    else:
        pl.when(count > 0)(run)

    if closing:
        for t in range(tiles):
            for h in range(group):
                slot = t * group + h
                obuf[pl.ds(t * TILE, TILE), h * HEAD : (h + 1) * HEAD] = (
                    (acc_ref[slot] / l_ref[slot]).astype(obuf.dtype).T
                )
        size = rows // pieces
        run_all([
            pltpu.make_async_copy(
                obuf.at[pl.ds(pl.multiple_of(((my_tp + k) % pieces) * size, size), size), :],
                outs[k], sems.at[k],
            )
            for k in range(pieces)
        ])


def attend(head, low, group, pieces, cp_size, far_stretches, bounds, starts, q_pair, messages, state=None, closing=True):
    opening = state is None
    rows = messages[-1].shape[0] // 2
    cols = group * HEAD
    tiles = rows // TILE
    stretches = len(messages) - (low == 0)
    high = low + stretches * tiles
    slots = (tiles + 1) * group
    held = [
        ((rows, cols), jnp.bfloat16),
        ((slots, 1, TILE), jnp.float32),
        ((slots, 1, TILE), jnp.float32),
        ((slots, HEAD, TILE), jnp.float32),
    ]
    scratch = [
        pltpu.VMEM((stretches * rows, HEAD), jnp.bfloat16),
        pltpu.VMEM((stretches * tiles, HEAD, TILE), jnp.bfloat16),
        pltpu.VMEM((2, group, 1, TILE), jnp.float32),
        pltpu.VMEM((group, TILE, TILE), jnp.float32),
        pltpu.VMEM((group, TILE, TILE), jnp.bfloat16),
        pltpu.VMEM((TILE, TILE), jnp.float32),
        pltpu.SMEM((40,), jnp.int32),
        pltpu.SMEM((40,), jnp.int32),
        pltpu.SMEM((40,), jnp.int32),
    ]
    outs = []
    if closing:
        scratch.append(pltpu.VMEM((rows, cols), jnp.bfloat16))
        outs = [jax.ShapeDtypeStruct((rows // pieces, cols), jnp.bfloat16)] * pieces
    scratch.append(pltpu.SemaphoreType.DMA((8,)))
    operands = [bounds, starts]
    specs = [scalars, fast]
    if opening:
        operands += list(q_pair)
        specs += [anywhere, fast]
    operands += messages
    specs += [fast] * len(messages)
    aliases = {}
    if opening and closing:
        scratch = [pltpu.VMEM(*h) for h in held] + scratch
    else:
        if not opening:
            for n in range(len(held)):
                aliases[len(operands) + n] = len(outs) + n
            operands += state
            specs += [fast] * len(held)
        outs = outs + [jax.ShapeDtypeStruct(*h) for h in held]
    return pl.pallas_call(
        functools.partial(
            attend_kernel, head, low, high, opening, closing, pieces, cp_size, far_stretches
        ),
        in_specs=specs,
        out_specs=[fast] * len(outs),
        out_shape=outs,
        scratch_shapes=scratch,
        input_output_aliases=aliases,
        compiler_params=pltpu.CompilerParams(vmem_limit_bytes=12 << 20),
    )(*operands)


def stretch_of(device, cp_size):
    return jnp.where(device % 2 == 0, device // 2, cp_size - 1 - device // 2)


def docs_kernel(rows, cp_size, lengths, bounds_ref, starts_ref):
    stretch = stretch_of(lax.axis_index("cp"), cp_size)
    origin = (stretch - 2) * rows
    tiles = rows // TILE
    pos = [
        2 * rows + t * TILE + lax.broadcasted_iota(jnp.int32, (8, TILE), 1) for t in range(tiles)
    ]

    def step(j, carry):
        end, edges, begins = carry
        end = end + lengths[j]
        edges = tuple(
            jnp.where(end <= 2 * rows + (n // 2) * TILE + (n % 2) * (TILE - 1), end, e)
            for n, e in enumerate(edges)
        )
        begins = tuple(jnp.where(p >= end, end, b) for p, b in zip(pos, begins))
        return end, edges, begins

    start = -origin
    edges = (start,) * (2 * tiles)
    begins = tuple(jnp.full((8, TILE), start, jnp.int32) for _ in range(tiles))
    _, edges, begins = lax.fori_loop(0, lengths.shape[0], step, (start, edges, begins), unroll=8)
    for n in range(2 * tiles):
        bounds_ref[n] = edges[n]
    for t in range(tiles):
        starts_ref[t] = begins[t][:1]


def docs(lengths, rows, cp_size):
    tiles = rows // TILE
    return pl.pallas_call(
        functools.partial(docs_kernel, rows, cp_size),
        in_specs=[scalars],
        out_specs=[scalars, fast],
        out_shape=[
            jax.ShapeDtypeStruct((2 * tiles,), jnp.int32),
            jax.ShapeDtypeStruct((tiles, 1, TILE), jnp.int32),
        ],
        compiler_params=pltpu.CompilerParams(vmem_limit_bytes=1 << 20),
    )(lengths)


def place_kernel(head, heads, *refs):
    pieces = len(refs) - 2 - (head > 0)
    out, sems = refs[-2:]
    _, cols = refs[0].shape
    t = lax.axis_index("tp")
    j = t % 2 + 2 * jnp.where(lax.axis_index("cp") % 2 == t // 2, 0, 1)
    run_all([
        pltpu.make_async_copy(
            refs[k],
            out.at[:, pl.ds(pl.multiple_of(((j + pieces - k) % pieces) * (heads * cols) + head * cols, cols), cols)],
            sems.at[k],
        )
        for k in range(pieces)
    ])


def place(head, heads, pieces, result):
    rows, cols = pieces[0].shape
    operands = [*pieces] + ([] if result is None else [result])
    return pl.pallas_call(
        functools.partial(place_kernel, head, heads),
        in_specs=[fast] * len(pieces) + [anywhere] * (result is not None),
        out_specs=anywhere,
        out_shape=jax.ShapeDtypeStruct((rows, cols * heads * len(pieces)), pieces[0].dtype),
        scratch_shapes=[pltpu.SemaphoreType.DMA((len(pieces),))],
        input_output_aliases={} if result is None else {len(operands) - 1: 0},
        compiler_params=pltpu.CompilerParams(vmem_limit_bytes=4 << 20),
    )(*operands)


def on_device(queries, keys, values, doc_lengths):
    tok_rows, q_cols = queries.shape
    kv_local = keys.shape[1] // HEAD
    group_cols = q_cols // kv_local
    cp_size = lax.axis_size("cp")
    tp_size = lax.axis_size("tp")

    swap = [(i, i ^ 1) for i in range(cp_size)]
    link = lambda s, d: (device_of(s, cp_size), device_of(s + d, cp_size))
    ahead = [link(s, 1) for s in range(cp_size - 1)]
    long_hops = [cp_size // 4 - 1, cp_size - 1 - cp_size // 4]
    handed = [link(s, 1) for s in range(cp_size - 1) if s not in long_hops]
    direct = [link(s - 1, 2) for s in long_hops]
    far_stretches = [s + 1 for s in long_hops]

    def route(k):
        pairs = []
        for c in range(cp_size):
            for t in range(tp_size):
                j = (t + k) % tp_size
                dest_c = c if j < 2 else c ^ 1
                dest_t = j % 2 + 2 * (c % 2)
                pairs.append((c * tp_size + t, dest_c * tp_size + dest_t))
        return pairs

    k_got = lax.ppermute(keys, "cp", swap)
    v_got = lax.ppermute(values, "cp", swap)
    q_got = lax.ppermute(queries, "cp", swap)
    bounds, starts = docs(doc_lengths, tok_rows, cp_size)
    messages = join(pltpu.with_memory_space_constraint(keys, pltpu.HBM), pltpu.with_memory_space_constraint(values, pltpu.HBM), k_got, v_got, bounds)

    near = [lax.ppermute(messages[h], "cp", ahead) for h in range(kv_local)]
    far = [lax.ppermute(messages[h], "cp", direct) for h in range(kv_local)]
    next_near = [lax.ppermute(near[h], "cp", handed) for h in range(kv_local)]
    group = group_cols // HEAD
    tiles = tok_rows // TILE
    q_pair = (pltpu.with_memory_space_constraint(queries, pltpu.HBM), q_got)
    received = []
    for h in range(kv_local):
        if h == 0:
            state = attend(h, 2 * tiles, group, tp_size, cp_size, far_stretches, bounds, starts, q_pair,
                          [messages[h]], closing=False)
            state = attend(h, tiles, group, tp_size, cp_size, far_stretches, bounds, starts, q_pair,
                          [near[h]], state=state, closing=False)
            out = attend(h, 0, group, tp_size, cp_size, far_stretches, bounds, starts, q_pair,
                        [far[h], next_near[h]], state=state)
        else:
            out = attend(h, 0, group, tp_size, cp_size, far_stretches, bounds, starts, q_pair,
                        [far[h], next_near[h], near[h], messages[h]])
        received.append([lax.ppermute(out[k], ("cp", "tp"), route(k)) for k in range(tp_size)])

    result = None
    for h in range(kv_local):
        result = place(h, kv_local, received[h], result)
    return result


def solution(mesh):
    in_specs = (P("cp", "tp"), P("cp", "tp"), P("cp", "tp"), P())
    out_specs = P(("cp", "tp"), None)
    return jax.shard_map(on_device, mesh=mesh, in_specs=in_specs, out_specs=out_specs, check_vma=False)
```
